16 devices in a mesh: dp: 1, tp: 16 (over x, y, z, core).
Axes of the slice: x: 2, y: 2, z: 2, core: 2. Of those that a mesh axis runs over, the one named last changes fastest.
Arguments:
- x: bfloat16 [2048, 14336], P(('dp', 'tp'))
- gain: bfloat16 [14336], replicated
- wq: bfloat16 [14336, 14336], P(None, 'tp')
- wk: bfloat16 [14336, 14336], P(None, 'tp')
- wv: bfloat16 [14336, 14336], P(None, 'tp')
- wo: bfloat16 [14336, 14336], P('tp')
Outputs:
- output: bfloat16 [2048, 14336], P(('dp', 'tp'))
All inputs are finite; a program needn't handle non-finite values.
Results may differ from the reference program's by a relative error of at most 0.012.
Values are sent between devices in bfloat16 or wider.
A program may use at most 2 GiB of HBM per device.

```python
import jax
import jax.numpy as jnp
from jax import lax

ROWS = 2048
D = 14336
HEADS = 112
KV_HEADS = 112
HEAD = 128
THETA = 10000


def setup_inputs(seed: int = 0, part: int = 0) -> dict:
    kx, kn, kq, kk, kv, ko = jax.random.split(jax.random.key(seed), 6)

    def weights(key, rows, columns):
        return jax.random.normal(key, (rows, columns), jnp.float32) * rows**-0.5

    drawn = {
        "x": jax.random.normal(jax.random.fold_in(kx, part), (ROWS, D), jnp.float32),
        "gain": 1 + 0.1 * jax.random.normal(kn, (D,), jnp.float32),
        "wq": 2 * weights(kq, D, HEADS * HEAD),
        "wk": 2 * weights(kk, D, KV_HEADS * HEAD),
        "wv": 4 * weights(kv, D, KV_HEADS * HEAD),
        "wo": weights(ko, HEADS * HEAD, D),
    }
    return {k: v.astype(jnp.bfloat16) for k, v in drawn.items()}


def normed(x, gain):
    wide = x.astype(jnp.float32)
    scale = lax.rsqrt(jnp.mean(wide * wide, -1, keepdims=True) + 1e-6)
    return (wide * scale * gain.astype(jnp.float32)).astype(jnp.bfloat16)


def turned(t, place, theta):
    half = t.shape[-1] // 2
    angle = place.astype(jnp.float32)[:, None] * theta ** (-jnp.arange(half, dtype=jnp.float32) / half)
    cos, sin = jnp.cos(angle)[:, None], jnp.sin(angle)[:, None]
    a, b = t[..., :half].astype(jnp.float32), t[..., half:].astype(jnp.float32)
    return jnp.concatenate([a * cos - b * sin, b * cos + a * sin], -1).astype(jnp.bfloat16)


def matmul(a, w):
    return jnp.dot(a, w, preferred_element_type=jnp.float32).astype(jnp.bfloat16)


def einsum(form, a, b):
    return jnp.einsum(form, a.astype(jnp.float32), b.astype(jnp.float32))


def attention(q, k, v):
    scores = einsum("tgsd,ugd->gstu", q, k) * q.shape[-1] ** -0.5
    token = jnp.arange(q.shape[0])
    scores = jnp.where(token[:, None] >= token, scores, -jnp.inf)
    weights = jax.nn.softmax(scores, -1).astype(jnp.bfloat16)
    return einsum("gstu,ugd->tgsd", weights, v).astype(jnp.bfloat16)


def reference(x, gain, wq, wk, wv, wo):
    a, place = normed(x, gain), jnp.arange(ROWS)
    q = turned(matmul(a, wq).reshape(ROWS, HEADS, HEAD), place, THETA).reshape(ROWS, KV_HEADS, -1, HEAD)
    k = turned(matmul(a, wk).reshape(ROWS, KV_HEADS, HEAD), place, THETA)
    v = matmul(a, wv).reshape(ROWS, KV_HEADS, HEAD)
    seen = attention(q, k, v).reshape(ROWS, HEADS * HEAD)
    return (x.astype(jnp.float32) + jnp.dot(seen, wo, preferred_element_type=jnp.float32)).astype(jnp.bfloat16)
```

```python
import functools

import jax
import jax.numpy as jnp
from jax import lax
from jax.experimental import pallas as pl
from jax.experimental.pallas import tpu as pltpu
from jax.sharding import PartitionSpec as P

NEG = -1e30
HIDDEN = 2 * NEG
LOG2E = 1.4426950408889634
VMEM = 56 * 2**20
HEAD = 128
THETA = 10000
BITS = {"x": 8, "y": 4, "z": 2, "core": 1}
AXES = ("x", "y", "z", "core")

PIECE = 1024
AHEAD = 4
STREAMS = (("xyz", 5), ("yzx", 5), ("zxy", 5), ("xyz", 5), ("yzx", 4), ("zxy", 4))
UNIT = 512


def _dot(a, b, ca, cb):
    return lax.dot_general(a, b, (((ca,), (cb,)), ((), ())), preferred_element_type=jnp.float32)


def normed(x, gain):
    wide = x.astype(jnp.float32)
    scale = lax.rsqrt(jnp.mean(wide * wide, -1, keepdims=True) + 1e-6)
    return (wide * scale * gain.astype(jnp.float32)).astype(jnp.bfloat16)


def _flip(place, weight):
    return place + weight * (1 - 2 * lax.rem(lax.div(place, weight), 2))


def _axes(piece):
    turns = [lax.rem(piece + n, 3) for n in range(3)]
    return [lax.div(8, 1 + r + lax.div(r, 2)) for r in turns]


PATHS = ((0,), (1,), (0, 1), (2,), (0, 2), (1, 2), (0, 1, 2))
ONWARD = {0: (2, 4), 1: (5,), 2: (6,)}


def _gather_project(h, wq, wk, wv, cos_ref, sin_ref, q_out, k_out, v_out, g, acc, wbuf, xbuf, stage, send, recv, core_send, core_recv,
                    wsem, xsem, osem, *, pieces, subs, ahead):
    me = lax.axis_index("tp")
    mate = _flip(me, 1)
    per, piece_cols = g.shape[2], g.shape[3]
    width = wq.shape[1]
    heads = width // HEAD
    blocks = xbuf.shape[1]

    barrier = pltpu.get_barrier_semaphore()
    for w in (8, 4, 2, 1):
        pl.semaphore_signal(barrier, inc=1, device_id={"tp": _flip(me, w)}, device_id_type=pl.DeviceIdType.MESH)
    pl.semaphore_wait(barrier, 4)

    def own(p):
        return h.at[:, pl.ds(pl.multiple_of(p * piece_cols, piece_cols), piece_cols)]

    def remote(src, dst, ssem, rsem, device):
        return pltpu.make_async_remote_copy(src_ref=src, dst_ref=dst, send_sem=ssem, recv_sem=rsem, device_id={"tp": device},
                                            device_id_type=pl.DeviceIdType.MESH)

    def block_of(place, p, n):
        w = _axes(p)
        for step in PATHS[n]:
            place = _flip(place, w[step])
        return place

    def link(p, n, block, mine=False):
        device = _flip(me, _axes(p)[PATHS[n][-1]])
        return remote(own(p) if mine else g.at[p, block], g.at[p, block], send.at[p, n], recv.at[p, n], device)

    def across(p, k, block, mine=False):
        return remote(own(p) if mine else g.at[p, block], g.at[p, block], core_send.at[p, k], core_recv.at[p, k], mate)

    def begin(p):
        for n in (0, 1, 3):
            link(p, n, me, True).start()
        across(p, 7, me, True).start()

    def arrive(p, n):
        block = block_of(me, p, n)
        link(p, n, block).wait_recv()
        for m in ONWARD.get(n, ()):
            link(p, m, block).start()
        across(p, n, block).start()

    def whole(p):
        for n in range(7):
            across(p, n, block_of(mate, p, n)).wait_recv()
        across(p, 7, mate).wait_recv()

    def weights(p):
        rows = pl.ds(pl.multiple_of(p * piece_cols, piece_cols), piece_cols)
        slot = lax.rem(p, 2)
        return [pltpu.make_async_copy(w.at[rows, :], wbuf.at[slot, :, n * width : (n + 1) * width], wsem.at[slot, n])
                for n, w in enumerate((wq, wk, wv))]

    def fetch(p, j):
        slot = j % 2
        for n in range(blocks):
            b = j * blocks + n

            @pl.when(b == me)
            def _():
                pltpu.make_async_copy(own(p), xbuf.at[slot, n], xsem.at[slot, n]).start()

            @pl.when(b != me)
            def _():
                pltpu.make_async_copy(g.at[p, b], xbuf.at[slot, n], xsem.at[slot, n]).start()

    def fetched(p, j):
        slot = j % 2
        for n in range(blocks):
            pltpu.make_async_copy(g.at[p, j * blocks + n], xbuf.at[slot, n], xsem.at[slot, n]).wait()

    def valid(p, f, *args):
        pl.when((p >= 0) & (p < pieces))(lambda: f(p, *args))

    for c in weights(0):
        c.start()
    acc[...] = jnp.zeros(acc.shape, jnp.float32)
    rows = blocks * per
    plan = {0: ((0, 3), (1, 3)), 1: ((2, 2), (6, 1)), 2: ((3, 2), (4, 2)), 3: ((5, 2),)}

    def step(i, _):
        t = i - ahead

        @pl.when(t >= 0)
        def _():
            for c in weights(t):
                c.wait()

            @pl.when(t + 1 < pieces)
            def _():
                for c in weights(t + 1):
                    c.start()

        for j in range(subs):
            if j == 0:
                valid(t + ahead, begin)
            for n, lag in plan[j]:
                valid(t + lag, arrive, n)
            if j == subs - 1:
                def ready(p):
                    whole(p)
                    fetch(p, 0)

                valid(t + 1, ready)

            @pl.when(t >= 0)
            def _():
                if j + 1 < subs:
                    fetch(t, j + 1)
                fetched(t, j)
                here = pl.ds(j * rows, rows)
                acc[here, :] += _dot(xbuf[j % 2].reshape(rows, piece_cols), wbuf[lax.rem(t, 2)], 1, 0)

        return ()

    lax.fori_loop(0, pieces + ahead, step, ())

    def outs(j):
        slot = lax.rem(j, 2)
        at = pl.ds(pl.multiple_of(j * per, per), per)
        return [pltpu.make_async_copy(stage.at[slot, n * heads : (n + 1) * heads], out.at[:, at, :], osem.at[slot, n])
                for n, out in enumerate((q_out, k_out, v_out))]

    def finish(j, _):
        @pl.when(j >= 2)
        def _():
            for c in outs(j - 2):
                c.wait()

        here = pl.ds(pl.multiple_of(j * per, per), per)
        cos, sin = cos_ref[here, :], sin_ref[here, :]
        for i in range(3 * heads):
            t = acc[here, i * HEAD : (i + 1) * HEAD].astype(jnp.bfloat16)
            if i < 2 * heads:
                wide = t.astype(jnp.float32)
                t = (wide * cos + pltpu.roll(wide, HEAD // 2, 1) * sin).astype(jnp.bfloat16)
            stage[lax.rem(j, 2), i] = t
        for c in outs(j):
            c.start()
        return ()

    group = g.shape[1]
    lax.fori_loop(0, group, finish, ())
    for j in (group - 2, group - 1):
        for c in outs(j):
            c.wait()

    def sent(p, _):
        for n in range(7):
            link(p, n, me).wait_send()
        for k in range(8):
            across(p, k, me).wait_send()
        return ()

    lax.fori_loop(0, pieces, sent, ())


def gather_project(h, wq, wk, wv, cos, sin, group):
    per, depth = h.shape
    width = wq.shape[1]
    heads = width // HEAD
    pieces, subs = depth // PIECE, 4
    blocks = group // subs
    anywhere, vmem = pl.BlockSpec(memory_space=pl.ANY), pl.BlockSpec(memory_space=pltpu.VMEM)
    out = jax.ShapeDtypeStruct((heads, group * per, HEAD), jnp.bfloat16)
    got = pl.pallas_call(
        functools.partial(_gather_project, pieces=pieces, subs=subs, ahead=AHEAD),
        in_specs=[anywhere] * 4 + [vmem] * 2,
        out_specs=[anywhere] * 4,
        out_shape=[out, out, out, jax.ShapeDtypeStruct((pieces, group, per, PIECE), jnp.bfloat16)],
        scratch_shapes=[
            pltpu.VMEM((group * per, 3 * width), jnp.float32),
            pltpu.VMEM((2, PIECE, 3 * width), jnp.bfloat16),
            pltpu.VMEM((2, blocks, per, PIECE), jnp.bfloat16),
            pltpu.VMEM((2, 3 * heads, per, HEAD), jnp.bfloat16),
            pltpu.SemaphoreType.DMA((pieces, 7)),
            pltpu.SemaphoreType.DMA((pieces, 7)),
            pltpu.SemaphoreType.DMA((pieces, 8)),
            pltpu.SemaphoreType.DMA((pieces, 8)),
            pltpu.SemaphoreType.DMA((2, 3)),
            pltpu.SemaphoreType.DMA((2, blocks)),
            pltpu.SemaphoreType.DMA((2, 3)),
        ],
        compiler_params=pltpu.CompilerParams(collective_id=0, has_side_effects=True, vmem_limit_bytes=VMEM),
        cost_estimate=pl.CostEstimate(
            flops=2 * group * per * depth * 3 * width, transcendentals=0, bytes_accessed=2 * (3 * wq.size + 3 * group * h.size)),
    )(h, wq, wk, wv, cos, sin)
    return got[:3]


def _attend(me_ref, q_ref, k_ref, v_ref, o_ref, top_s, mix_s, gap_s, *, scale, bq, bk):
    heads = q_ref.shape[0]
    iq = pl.program_id(0)
    e = scale * LOG2E
    top_s[...] = jnp.full(top_s.shape, NEG, jnp.float32)
    mix_s[...] = jnp.zeros(mix_s.shape, jnp.float32)
    gap_s[...] = lax.broadcasted_iota(jnp.int32, (bk, bq), 1) - lax.broadcasted_iota(jnp.int32, (bk, bq), 0)
    ones = jnp.ones((8, bk), jnp.bfloat16)

    def block(j, masked):
        here = pl.ds(j * bk, bk)
        scores = [_dot(k_ref[i, here, :], q_ref[i], 1, 1) for i in range(heads)]
        ok = gap_s[...] >= j * bk - iq * bq if masked else None
        weights, keeps = [], []
        for i, s in enumerate(scores):
            if masked:
                s = jnp.where(ok, s, HIDDEN)
            old = top_s[i : i + 1, :]
            top = jnp.maximum(old, s.max(axis=0, keepdims=True))
            top_s[i : i + 1, :] = top
            weights.append(jnp.exp2((s - top) * e).astype(jnp.bfloat16))
            keeps.append(jnp.exp2((old - top) * e))
        for i, (p, keep) in enumerate(zip(weights, keeps)):
            values = jnp.concatenate([v_ref[i, here, :].T, ones], axis=0)
            mix_s[i] = mix_s[i] * keep + _dot(values, p, 1, 0)

    whole = lax.div(iq * bq, bk)
    lax.fori_loop(0, whole, lambda j, _: block(j, False), None)
    lax.fori_loop(whole, lax.div(iq * bq + bq, bk), lambda j, _: block(j, True), None)

    low = lax.rem(me_ref[0], bq // 128)
    for i in range(heads):
        out = (mix_s[i, :HEAD, :] * (1 / mix_s[i, HEAD : HEAD + 1, :])).T.astype(jnp.bfloat16)
        for n in range(bq // 128):
            o_ref[jnp.bitwise_xor(low, n), :, i * HEAD : (i + 1) * HEAD] = out[n * 128 : (n + 1) * 128]


def attend(q, k, v, me, bq=512, bk=512):
    heads, tokens, _ = q.shape
    per = bq // 128
    whole = pl.BlockSpec((heads, tokens, HEAD), lambda i, me: (0, 0, 0))
    return pl.pallas_call(
        functools.partial(_attend, scale=HEAD**-0.5, bq=bq, bk=bk),
        grid_spec=pltpu.PrefetchScalarGridSpec(
            num_scalar_prefetch=1,
            grid=(tokens // bq,),
            in_specs=[pl.BlockSpec((heads, bq, HEAD), lambda i, me: (0, i, 0)), whole, whole],
            out_specs=pl.BlockSpec((per, 128, heads * HEAD), lambda i, me: (jnp.bitwise_xor(i, lax.div(me[0], per)), 0, 0)),
            scratch_shapes=[pltpu.VMEM((heads, bq), jnp.float32), pltpu.VMEM((heads, HEAD + 8, bq), jnp.float32),
                            pltpu.VMEM((bk, bq), jnp.int32)],
        ),
        out_shape=jax.ShapeDtypeStruct((tokens // 128, 128, heads * HEAD), jnp.bfloat16),
        compiler_params=pltpu.CompilerParams(dimension_semantics=("arbitrary",), vmem_limit_bytes=VMEM),
        cost_estimate=pl.CostEstimate(
            flops=2 * heads * tokens * tokens * HEAD, transcendentals=heads * tokens * tokens // 2, bytes_accessed=8 * q.size),
    )(me, q, k, v)


def _term(b_ref, wo_ref, *rest):
    o_ref, adds = rest[-1], rest[:-1]
    rows = b_ref[...].reshape(-1, b_ref.shape[-1])
    total = _dot(rows, wo_ref[...], 1, 0)
    for r in adds:
        total += r[...].reshape(total.shape).astype(jnp.float32)
    o_ref[...] = total.astype(o_ref.dtype).reshape(o_ref.shape)


def term(seen, wo, first, units, fixed, adds):
    size = tuple(1 if n in fixed else 2 for n in AXES)
    width = seen.shape[-1]

    def at(shape):
        return tuple(fixed[n] if n in fixed and d == 2 else 0 for n, d in zip(AXES, shape))

    rows = 128 * size[0] * size[1] * size[2] * size[3]
    specs = [pl.BlockSpec((*size, 128, width), lambda i: (*at(seen.shape[:4]), 0, 0)), pl.BlockSpec((width, UNIT), lambda i: (0, first + i))]
    for r in adds:
        specs.append(pl.BlockSpec((*size, 128, UNIT), lambda i, s=r.shape[:4]: (*at(s), 0, i)))
    return pl.pallas_call(
        _term,
        grid=(units,),
        in_specs=specs,
        out_specs=pl.BlockSpec((*size, 128, UNIT), lambda i: (0, 0, 0, 0, 0, i)),
        out_shape=jax.ShapeDtypeStruct((*size, 128, units * UNIT), jnp.bfloat16),
        compiler_params=pltpu.CompilerParams(dimension_semantics=("arbitrary",), vmem_limit_bytes=VMEM // 2),
        cost_estimate=pl.CostEstimate(
            flops=2 * rows * width * units * UNIT, transcendentals=0,
            bytes_accessed=2 * (rows * width + width * units * UNIT + (1 + len(adds)) * rows * units * UNIT)),
    )(seen, wo, *adds)


def _last(b_ref, wo_ref, x_ref, *rest, carried):
    o_ref, adds = rest[-1], rest[:-2] if carried else rest[:-1]
    total = _dot(b_ref[...].reshape(128, -1), wo_ref[...], 1, 0)
    for r in adds:
        total += r[...].reshape(total.shape).astype(jnp.float32)
    o_ref[...] = (x_ref[...].astype(jnp.float32) + total).astype(o_ref.dtype)


def last(seen, wo, x, first, units, adds, y):
    width = seen.shape[-1]
    here = pl.BlockSpec((128, UNIT), lambda i: (0, first + i))
    specs = [pl.BlockSpec((1, 1, 1, 1, 128, width), lambda i: (0,) * 6), pl.BlockSpec((width, UNIT), lambda i: (0, first + i)), here]
    specs += [pl.BlockSpec((1, 1, 1, 1, 128, UNIT), lambda i: (0, 0, 0, 0, 0, i)) for _ in adds]
    args = [seen, wo, x, *adds]
    if y is not None:
        specs.append(pl.BlockSpec(memory_space=pl.ANY))
        args.append(y)
    return pl.pallas_call(
        functools.partial(_last, carried=y is not None),
        grid=(units,),
        in_specs=specs,
        out_specs=here,
        out_shape=jax.ShapeDtypeStruct(x.shape, x.dtype),
        input_output_aliases={} if y is None else {len(args) - 1: 0},
        compiler_params=pltpu.CompilerParams(dimension_semantics=("arbitrary",), vmem_limit_bytes=VMEM // 2),
        cost_estimate=pl.CostEstimate(
            flops=2 * 128 * width * units * UNIT, transcendentals=0,
            bytes_accessed=2 * (width * units * UNIT + (2 + len(adds)) * 128 * units * UNIT)),
    )(*args)


def swap(t, axis):
    return lax.ppermute(t, "tp", [(i, i ^ BITS[axis]) for i in range(16)])


def solution(mesh):
    group = mesh.shape["tp"]

    def step(x, gain, wq, wk, wv, wo):
        per, depth = x.shape
        me = lax.axis_index("tp")
        half = HEAD // 2
        angle = jnp.arange(group * per).astype(jnp.float32)[:, None] * THETA ** (-jnp.arange(half, dtype=jnp.float32) / half)
        cos, sin = jnp.cos(angle), jnp.sin(angle)
        q, k, v = gather_project(
            normed(x, gain), wq, wk, wv, jnp.concatenate([cos, cos], 1), jnp.concatenate([-sin, sin], 1), group)
        seen = attend(q, k, v, me.astype(jnp.int32).reshape(1))
        seen = seen.reshape(2, 2, 2, 2, per, -1)

        firsts = [sum(u for _, u in STREAMS[:n]) for n in range(len(STREAMS))]
        state = [(order, first, units) for (order, units), first in zip(STREAMS, firsts)]
        near, far, r1, r2, r3 = {}, {}, {}, {}, {}
        for n, (o, f, u) in enumerate(state):
            far[n] = swap(term(seen, wo, f, u, {"core": 1, o[0]: 1}, []), "core")
        for n, (o, f, u) in enumerate(state):
            r1[n] = swap(term(seen, wo, f, u, {"core": 0, o[0]: 1}, [far[n]]), o[0])
        for n, (o, f, u) in enumerate(state):
            near[n] = swap(term(seen, wo, f, u, {"core": 1, o[0]: 0}, []), "core")
        for n, (o, f, u) in enumerate(state):
            r2[n] = swap(term(seen, wo, f, u, {"core": 0, o[0]: 0, o[1]: 1}, [near[n], r1[n]]), o[1])
        for n, (o, f, u) in enumerate(state):
            r3[n] = swap(term(seen, wo, f, u, {"core": 0, o[0]: 0, o[1]: 0, o[2]: 1}, [near[n], r1[n], r2[n]]), o[2])
        y = None
        for n, (o, f, u) in enumerate(state):
            y = last(seen, wo, x, f, u, [near[n], r1[n], r2[n], r3[n]], y)
        return y

    tokens, columns = P(("dp", "tp"), None), P(None, "tp")
    return jax.shard_map(
        step,
        mesh=mesh,
        in_specs=(tokens, P(None), columns, columns, columns, P("tp", None)),
        out_specs=tokens,
        check_vma=False,
    )
```

```python
import functools

import jax
import jax.numpy as jnp
from jax import lax
from jax.experimental import pallas as pl
from jax.experimental.pallas import tpu as pltpu
from jax.sharding import PartitionSpec as P

NEG = -1e30
HIDDEN = 2 * NEG
LOG2E = 1.4426950408889634
VMEM = 56 * 2**20
HEAD = 128
THETA = 10000
PIECE = 1024
AHEAD = 4
TURN = 512
LAGS = (0, 2, 6, 9, 12)
SLOTS = (3, 6, 4, 4, 2)


def _dot(a, b, ca, cb):
    return lax.dot_general(a, b, (((ca,), (cb,)), ((), ())), preferred_element_type=jnp.float32)


def normed(x, gain):
    wide = x.astype(jnp.float32)
    scale = lax.rsqrt(jnp.mean(wide * wide, -1, keepdims=True) + 1e-6)
    return (wide * scale * gain.astype(jnp.float32)).astype(jnp.bfloat16)


def _flip(place, weight):
    return place + weight * (1 - 2 * lax.rem(lax.div(place, weight), 2))


def _axes(piece):
    turns = [lax.rem(piece + n, 3) for n in range(3)]
    return [lax.div(8, 1 + r + lax.div(r, 2)) for r in turns]


PATHS = ((0,), (1,), (0, 1), (2,), (0, 2), (1, 2), (0, 1, 2))
ONWARD = {0: (2, 4), 1: (5,), 2: (6,)}


def _gather_project(h, wq, wk, wv, cos_ref, sin_ref, q_out, k_out, v_out, g, acc, wbuf, xbuf, stage, send, recv, core_send, core_recv,
                    wsem, xsem, osem, *, pieces, subs, ahead):
    me = lax.axis_index("tp")
    mate = _flip(me, 1)
    per, piece_cols = g.shape[2], g.shape[3]
    width = wq.shape[1]
    heads = width // HEAD
    blocks = xbuf.shape[1]

    barrier = pltpu.get_barrier_semaphore()
    for w in (8, 4, 2, 1):
        pl.semaphore_signal(barrier, inc=1, device_id={"tp": _flip(me, w)}, device_id_type=pl.DeviceIdType.MESH)
    pl.semaphore_wait(barrier, 4)

    def own(p):
        return h.at[:, pl.ds(pl.multiple_of(p * piece_cols, piece_cols), piece_cols)]

    def remote(src, dst, ssem, rsem, device):
        return pltpu.make_async_remote_copy(src_ref=src, dst_ref=dst, send_sem=ssem, recv_sem=rsem, device_id={"tp": device},
                                            device_id_type=pl.DeviceIdType.MESH)

    def block_of(place, p, n):
        w = _axes(p)
        for step in PATHS[n]:
            place = _flip(place, w[step])
        return place

    def link(p, n, block, mine=False):
        device = _flip(me, _axes(p)[PATHS[n][-1]])
        return remote(own(p) if mine else g.at[p, block], g.at[p, block], send.at[p, n], recv.at[p, n], device)

    def across(p, k, block, mine=False):
        return remote(own(p) if mine else g.at[p, block], g.at[p, block], core_send.at[p, k], core_recv.at[p, k], mate)

    def begin(p):
        for n in (0, 1, 3):
            link(p, n, me, True).start()
        across(p, 7, me, True).start()

    def arrive(p, n):
        block = block_of(me, p, n)
        link(p, n, block).wait_recv()
        for m in ONWARD.get(n, ()):
            link(p, m, block).start()
        across(p, n, block).start()

    def whole(p):
        for n in range(7):
            across(p, n, block_of(mate, p, n)).wait_recv()
        across(p, 7, mate).wait_recv()

    def weights(p):
        rows = pl.ds(pl.multiple_of(p * piece_cols, piece_cols), piece_cols)
        slot = lax.rem(p, 2)
        return [pltpu.make_async_copy(w.at[rows, :], wbuf.at[slot, :, n * width : (n + 1) * width], wsem.at[slot, n])
                for n, w in enumerate((wq, wk, wv))]

    def fetch(p, j):
        slot = j % 2
        for n in range(blocks):
            b = j * blocks + n

            @pl.when(b == me)
            def _():
                pltpu.make_async_copy(own(p), xbuf.at[slot, n], xsem.at[slot, n]).start()

            @pl.when(b != me)
            def _():
                pltpu.make_async_copy(g.at[p, b], xbuf.at[slot, n], xsem.at[slot, n]).start()

    def fetched(p, j):
        slot = j % 2
        for n in range(blocks):
            pltpu.make_async_copy(g.at[p, j * blocks + n], xbuf.at[slot, n], xsem.at[slot, n]).wait()

    def valid(p, f, *args):
        pl.when((p >= 0) & (p < pieces))(lambda: f(p, *args))

    for c in weights(0):
        c.start()
    acc[...] = jnp.zeros(acc.shape, jnp.float32)
    rows = blocks * per
    plan = {0: ((0, 3), (1, 3)), 1: ((2, 2), (6, 1)), 2: ((3, 2), (4, 2)), 3: ((5, 2),)}

    def step(i, _):
        t = i - ahead

        @pl.when(t >= 0)
        def _():
            for c in weights(t):
                c.wait()

            @pl.when(t + 1 < pieces)
            def _():
                for c in weights(t + 1):
                    c.start()

        for j in range(subs):
            if j == 0:
                valid(t + ahead, begin)
            for n, lag in plan[j]:
                valid(t + lag, arrive, n)
            if j == subs - 1:
                def ready(p):
                    whole(p)
                    fetch(p, 0)

                valid(t + 1, ready)

            @pl.when(t >= 0)
            def _():
                if j + 1 < subs:
                    fetch(t, j + 1)
                fetched(t, j)
                here = pl.ds(j * rows, rows)
                acc[here, :] += _dot(xbuf[j % 2].reshape(rows, piece_cols), wbuf[lax.rem(t, 2)], 1, 0)

        return ()

    lax.fori_loop(0, pieces + ahead, step, ())

    def outs(j):
        slot = lax.rem(j, 2)
        at = pl.ds(pl.multiple_of(j * per, per), per)
        return [pltpu.make_async_copy(stage.at[slot, n * heads : (n + 1) * heads], out.at[:, at, :], osem.at[slot, n])
                for n, out in enumerate((q_out, k_out, v_out))]

    def finish(j, _):
        @pl.when(j >= 2)
        def _():
            for c in outs(j - 2):
                c.wait()

        here = pl.ds(pl.multiple_of(j * per, per), per)
        cos, sin = cos_ref[here, :], sin_ref[here, :]
        for i in range(3 * heads):
            t = acc[here, i * HEAD : (i + 1) * HEAD].astype(jnp.bfloat16)
            if i < 2 * heads:
                wide = t.astype(jnp.float32)
                t = (wide * cos + pltpu.roll(wide, HEAD // 2, 1) * sin).astype(jnp.bfloat16)
            stage[lax.rem(j, 2), i] = t
        for c in outs(j):
            c.start()
        return ()

    group = g.shape[1]
    lax.fori_loop(0, group, finish, ())
    for j in (group - 2, group - 1):
        for c in outs(j):
            c.wait()

    def sent(p, _):
        for n in range(7):
            link(p, n, me).wait_send()
        for k in range(8):
            across(p, k, me).wait_send()
        return ()

    lax.fori_loop(0, pieces, sent, ())


def gather_project(h, wq, wk, wv, cos, sin, group):
    per, depth = h.shape
    width = wq.shape[1]
    heads = width // HEAD
    pieces, subs = depth // PIECE, 4
    blocks = group // subs
    anywhere, vmem = pl.BlockSpec(memory_space=pl.ANY), pl.BlockSpec(memory_space=pltpu.VMEM)
    out = jax.ShapeDtypeStruct((heads, group * per, HEAD), jnp.bfloat16)
    got = pl.pallas_call(
        functools.partial(_gather_project, pieces=pieces, subs=subs, ahead=AHEAD),
        in_specs=[anywhere] * 4 + [vmem] * 2,
        out_specs=[anywhere] * 4,
        out_shape=[out, out, out, jax.ShapeDtypeStruct((pieces, group, per, PIECE), jnp.bfloat16)],
        scratch_shapes=[
            pltpu.VMEM((group * per, 3 * width), jnp.float32),
            pltpu.VMEM((2, PIECE, 3 * width), jnp.bfloat16),
            pltpu.VMEM((2, blocks, per, PIECE), jnp.bfloat16),
            pltpu.VMEM((2, 3 * heads, per, HEAD), jnp.bfloat16),
            pltpu.SemaphoreType.DMA((pieces, 7)),
            pltpu.SemaphoreType.DMA((pieces, 7)),
            pltpu.SemaphoreType.DMA((pieces, 8)),
            pltpu.SemaphoreType.DMA((pieces, 8)),
            pltpu.SemaphoreType.DMA((2, 3)),
            pltpu.SemaphoreType.DMA((2, blocks)),
            pltpu.SemaphoreType.DMA((2, 3)),
        ],
        compiler_params=pltpu.CompilerParams(collective_id=0, has_side_effects=True, vmem_limit_bytes=VMEM),
        cost_estimate=pl.CostEstimate(
            flops=2 * group * per * depth * 3 * width, transcendentals=0, bytes_accessed=2 * (3 * wq.size + 3 * group * h.size)),
    )(h, wq, wk, wv, cos, sin)
    return got[:3]


def _attend(me_ref, q_ref, k_ref, v_ref, o_ref, top_s, mix_s, gap_s, *, scale, bq, bk):
    heads = q_ref.shape[0]
    iq = pl.program_id(0)
    e = scale * LOG2E
    top_s[...] = jnp.full(top_s.shape, NEG, jnp.float32)
    mix_s[...] = jnp.zeros(mix_s.shape, jnp.float32)
    gap_s[...] = lax.broadcasted_iota(jnp.int32, (bk, bq), 1) - lax.broadcasted_iota(jnp.int32, (bk, bq), 0)
    ones = jnp.ones((8, bk), jnp.bfloat16)

    def block(j, masked):
        here = pl.ds(j * bk, bk)
        scores = [_dot(k_ref[i, here, :], q_ref[i], 1, 1) for i in range(heads)]
        ok = gap_s[...] >= j * bk - iq * bq if masked else None
        weights, keeps = [], []
        for i, s in enumerate(scores):
            if masked:
                s = jnp.where(ok, s, HIDDEN)
            old = top_s[i : i + 1, :]
            top = jnp.maximum(old, s.max(axis=0, keepdims=True))
            top_s[i : i + 1, :] = top
            weights.append(jnp.exp2((s - top) * e).astype(jnp.bfloat16))
            keeps.append(jnp.exp2((old - top) * e))
        for i, (p, keep) in enumerate(zip(weights, keeps)):
            values = jnp.concatenate([v_ref[i, here, :].T, ones], axis=0)
            mix_s[i] = mix_s[i] * keep + _dot(values, p, 1, 0)

    whole = lax.div(iq * bq, bk)
    lax.fori_loop(0, whole, lambda j, _: block(j, False), None)
    lax.fori_loop(whole, lax.div(iq * bq + bq, bk), lambda j, _: block(j, True), None)

    low = lax.rem(me_ref[0], bq // 128)
    for i in range(heads):
        out = (mix_s[i, :HEAD, :] * (1 / mix_s[i, HEAD : HEAD + 1, :])).T.astype(jnp.bfloat16)
        for n in range(bq // 128):
            o_ref[jnp.bitwise_xor(low, n), :, i * HEAD : (i + 1) * HEAD] = out[n * 128 : (n + 1) * 128]


def attend(q, k, v, me, bq=512, bk=512):
    heads, tokens, _ = q.shape
    per = bq // 128
    whole = pl.BlockSpec((heads, tokens, HEAD), lambda i, me: (0, 0, 0))
    return pl.pallas_call(
        functools.partial(_attend, scale=HEAD**-0.5, bq=bq, bk=bk),
        grid_spec=pltpu.PrefetchScalarGridSpec(
            num_scalar_prefetch=1,
            grid=(tokens // bq,),
            in_specs=[pl.BlockSpec((heads, bq, HEAD), lambda i, me: (0, i, 0)), whole, whole],
            out_specs=pl.BlockSpec((per, 128, heads * HEAD), lambda i, me: (jnp.bitwise_xor(i, lax.div(me[0], per)), 0, 0)),
            scratch_shapes=[pltpu.VMEM((heads, bq), jnp.float32), pltpu.VMEM((heads, HEAD + 8, bq), jnp.float32),
                            pltpu.VMEM((bk, bq), jnp.int32)],
        ),
        out_shape=jax.ShapeDtypeStruct((tokens // 128, 128, heads * HEAD), jnp.bfloat16),
        compiler_params=pltpu.CompilerParams(dimension_semantics=("arbitrary",), vmem_limit_bytes=VMEM),
        cost_estimate=pl.CostEstimate(
            flops=2 * heads * tokens * tokens * HEAD, transcendentals=heads * tokens * tokens // 2, bytes_accessed=8 * q.size),
    )(me, q, k, v)


COUNT = (8, 4, 2, 1, 1)


def _project_scatter(seen, wo, x, y, r0, r1, r2, r3, wbuf, f0, f1, f2, f3, fx, s0, s1, s2, s3, s4, wsem, fsem, xsem, send, ysem, q0, q1, q2,
                     q3, *, pieces, lags, slots, early):
    me = lax.axis_index("tp")
    cols = wbuf.shape[2]
    arrived, fetches, stages, recv = (r0, r1, r2, r3), (f0, f1, f2, f3), (s0, s1, s2, s3, s4), (q0, q1, q2, q3)

    barrier = pltpu.get_barrier_semaphore()
    for w in (8, 4, 2, 1):
        pl.semaphore_signal(barrier, inc=1, device_id={"tp": _flip(me, w)}, device_id_type=pl.DeviceIdType.MESH)
    pl.semaphore_wait(barrier, 4)

    def here(p):
        return pl.ds(pl.multiple_of(p * cols, cols), cols)

    def weight(p):
        return pltpu.make_async_copy(wo.at[:, here(p)], wbuf.at[p], wsem.at[p])

    def out(p, k):
        slot = lax.rem(p, slots[k])
        if k == 4:
            return pltpu.make_async_copy(stages[4].at[slot], y.at[:, here(p)], ysem.at[slot])
        device = _flip(me, 1 if k == 0 else _axes(p)[k - 1])
        return pltpu.make_async_remote_copy(
            src_ref=stages[k].at[slot], dst_ref=arrived[k].at[p], send_sem=send.at[k, slot], recv_sem=recv[k].at[p],
            device_id={"tp": device}, device_id_type=pl.DeviceIdType.MESH)

    def share(k):
        first = COUNT[k] if k < 4 else 0
        return first, COUNT[k]

    def fetch(p, k):
        first, n = share(k)
        slot = lax.rem(p, 2)
        got = [pltpu.make_async_copy(arrived[m].at[p, first : first + n], fetches[m].at[slot, first : first + n], fsem.at[k, m, slot])
               for m in range(k)]
        if k == 4:
            got.append(pltpu.make_async_copy(x.at[:, here(p)], fx.at[slot], xsem.at[slot]))
        return got

    def ready(p, k):
        out(p, k - 1).wait_recv()
        for c in fetch(p, k):
            c.start()

    def work(p, k):
        first, n = share(k)
        w = _axes(p)
        js = []
        for i in range(n):
            i += first if k else 0
            if k == 0:
                js.append(1 + (i // 4) * w[0] + (i // 2 % 2) * w[1] + (i % 2) * w[2])
            else:
                js.append((i // 4) * w[0] + (i // 2 % 2) * w[1] + (i % 2) * w[2])
        rows = jnp.concatenate([seen[j] for j in js], axis=0) if n > 1 else seen[js[0]]
        total = _dot(rows, wbuf[p], 1, 0)
        slot = lax.rem(p, 2)
        if k:
            for c in fetch(p, k):
                c.wait()
            for m in range(k):
                total += fetches[m][slot, first : first + n].reshape(total.shape).astype(jnp.float32)
        if k == 4:
            total = fx[slot].astype(jnp.float32) + total

        @pl.when(p >= slots[k])
        def _():
            c = out(p - slots[k], k)
            c.wait() if k == 4 else c.wait_send()

        at = stages[k].at[lax.rem(p, slots[k])]
        at[...] = total.astype(jnp.bfloat16).reshape(at.shape)
        out(p, k).start()

    def valid(p, f, *args):
        pl.when((p >= 0) & (p < pieces))(lambda: f(p, *args))

    for p in range(early):
        weight(p).start()

    def step(i, _):
        for k in (3, 2, 1, 4):
            valid(i - lags[k], work, k)
        for k in (4, 3, 2, 1):
            valid(i + 1 - lags[k], ready, k)

        def begin(p):
            pl.when(p + early < pieces)(lambda: weight(p + early).start())
            weight(p).wait()
            work(p, 0)

        valid(i, begin)
        return ()

    lax.fori_loop(0, pieces + lags[4], step, ())
    for k in range(5):
        for p in range(pieces - slots[k], pieces):
            c = out(p, k)
            c.wait() if k == 4 else c.wait_send()


def project_scatter(seen, wo, x):
    per, width = seen.shape[1:]
    depth = wo.shape[1]
    pieces = depth // TURN
    anywhere, vmem = pl.BlockSpec(memory_space=pl.ANY), pl.BlockSpec(memory_space=pltpu.VMEM)
    arrivals = [jax.ShapeDtypeStruct((pieces, n, per, TURN), jnp.bfloat16) for n in COUNT[:4]]
    got = pl.pallas_call(
        functools.partial(_project_scatter, pieces=pieces, lags=LAGS, slots=SLOTS, early=4),
        in_specs=[vmem, anywhere, anywhere],
        out_specs=[anywhere] * 5,
        out_shape=[jax.ShapeDtypeStruct(x.shape, x.dtype), *arrivals],
        scratch_shapes=[pltpu.VMEM((pieces, width, TURN), jnp.bfloat16)]
        + [pltpu.VMEM((2, n, per, TURN), jnp.bfloat16) for n in COUNT[:4]]
        + [pltpu.VMEM((2, per, TURN), jnp.bfloat16)]
        + [pltpu.VMEM((slots, n, per, TURN), jnp.bfloat16) for slots, n in zip(SLOTS[:4], COUNT[:4])]
        + [pltpu.VMEM((SLOTS[4], per, TURN), jnp.bfloat16)]
        + [pltpu.SemaphoreType.DMA((pieces,)), pltpu.SemaphoreType.DMA((5, 4, 2)), pltpu.SemaphoreType.DMA((2,)),
           pltpu.SemaphoreType.DMA((4, max(SLOTS))), pltpu.SemaphoreType.DMA((SLOTS[4],))]
        + [pltpu.SemaphoreType.DMA((pieces,)) for _ in range(4)],
        compiler_params=pltpu.CompilerParams(collective_id=1, has_side_effects=True, vmem_limit_bytes=VMEM),
        cost_estimate=pl.CostEstimate(flops=2 * 16 * per * width * depth, transcendentals=0, bytes_accessed=2 * (wo.size + 32 * x.size)),
    )(seen, wo, x)
    return got[0]


def solution(mesh):
    group = mesh.shape["tp"]

    def step(x, gain, wq, wk, wv, wo):
        per, depth = x.shape
        me = lax.axis_index("tp")
        half = HEAD // 2
        angle = jnp.arange(group * per).astype(jnp.float32)[:, None] * THETA ** (-jnp.arange(half, dtype=jnp.float32) / half)
        cos, sin = jnp.cos(angle), jnp.sin(angle)
        q, k, v = gather_project(
            normed(x, gain), wq, wk, wv, jnp.concatenate([cos, cos], 1), jnp.concatenate([-sin, sin], 1), group)
        seen = attend(q, k, v, me.astype(jnp.int32).reshape(1))
        return project_scatter(seen, wo, x)

    tokens, columns = P(("dp", "tp"), None), P(None, "tp")
    return jax.shard_map(
        step,
        mesh=mesh,
        in_specs=(tokens, P(None), columns, columns, columns, P("tp", None)),
        out_specs=tokens,
        check_vma=False,
    )
```

```python
import functools

import jax
import jax.numpy as jnp
from jax import lax
from jax.experimental import pallas as pl
from jax.experimental.pallas import tpu as pltpu
from jax.sharding import PartitionSpec as P

NEG = -1e30
HIDDEN = 2 * NEG
LOG2E = 1.4426950408889634
VMEM = 56 * 2**20
HEAD = 128
THETA = 10000
SPAN = 1024
PIECE = 512
PARTS = (((0,), (1,)), ((2,), (0, 1)), ((1, 2), (0, 2)), ((0, 1, 2),))
SUBS = 4
AHEAD = {"own": 16, 0: 11, 1: 11, 2: 7, 6: 3, 3: 8, 4: 7, 5: 6}
TURN = 512
LAGS = (0, 2, 6, 9, 12)
SLOTS = (3, 6, 4, 4, 2)


def _dot(a, b, ca, cb):
    return lax.dot_general(a, b, (((ca,), (cb,)), ((), ())), preferred_element_type=jnp.float32)


def normed(x, gain):
    wide = x.astype(jnp.float32)
    scale = lax.rsqrt(jnp.mean(wide * wide, -1, keepdims=True) + 1e-6)
    return (wide * scale * gain.astype(jnp.float32)).astype(jnp.bfloat16)


def _flip(place, weight):
    return place + weight * (1 - 2 * lax.rem(lax.div(place, weight), 2))


def _axes(piece):
    turns = [lax.rem(piece + n, 3) for n in range(3)]
    return [lax.div(8, 1 + r + lax.div(r, 2)) for r in turns]


PATHS = ((0,), (1,), (0, 1), (2,), (0, 2), (1, 2), (0, 1, 2))
ONWARD = {0: (2, 4), 1: (5,), 2: (6,)}


def _gather_project(h, wq, wk, wv, near_ref, far_ref, q_out, k_out, v_out, g, acc, wbuf, xbuf, stage, send, recv, core_send, core_recv,
                    wsem, xsem, osem, *, pieces, before):
    me = lax.axis_index("tp")
    mate = _flip(me, 1)
    spans, group, per, _ = g.shape
    split = pieces // spans
    turn = SUBS // split
    width = wq.shape[1]
    heads = width // HEAD
    core = lax.rem(me, 2)

    barrier = pltpu.get_barrier_semaphore()
    for w in (8, 4, 2, 1):
        pl.semaphore_signal(barrier, inc=1, device_id={"tp": _flip(me, w)}, device_id_type=pl.DeviceIdType.MESH)
    pl.semaphore_wait(barrier, 4)

    def own(p, size=PIECE):
        return h.at[:, pl.ds(pl.multiple_of(p * size, size), size)]

    def held(p, block):
        return g.at[lax.div(p, split), block, :, pl.ds(pl.multiple_of(lax.rem(p, split) * PIECE, PIECE), PIECE)]

    def remote(src, dst, ssem, rsem, device):
        return pltpu.make_async_remote_copy(src_ref=src, dst_ref=dst, send_sem=ssem, recv_sem=rsem, device_id={"tp": device},
                                            device_id_type=pl.DeviceIdType.MESH)

    def block_of(place, p, n):
        w = _axes(p)
        for step in PATHS[n]:
            place = _flip(place, w[step])
        return place

    def link(p, n, block, mine=False):
        device = _flip(me, _axes(p)[PATHS[n][-1]])
        return remote(own(p) if mine else held(p, block), held(p, block), send.at[p, n], recv.at[p, n], device)

    def across(p, k, block, mine=False):
        return remote(own(p) if mine else held(p, block), held(p, block), core_send.at[p, k], core_recv.at[p, k], mate)

    def begin(p):
        for n in (0, 1, 3):
            link(p, n, me, True).start()

    def arrive(p, n):
        block = block_of(me, p, n)
        link(p, n, block).wait_recv()
        for m in ONWARD.get(n, ()):
            link(p, m, block).start()
        across(p, n, block).start()

    def beyond(place, axes):
        for axis in axes:
            place = _flip(place, (8, 4, 2)[axis])
        return place

    def number(p, axes):
        if len(axes) == 3:
            return 6
        axis = axes[0] if len(axes) == 1 else 3 - sum(axes)
        turn = lax.rem(axis + 3 - lax.rem(p, 3), 3)
        bend = turn + lax.div(turn, 2)
        return bend if len(axes) == 1 else 5 - bend

    def mates(t, k, place):
        for n in range(split):
            across(t * split + n, k if isinstance(k, int) else number(t * split + n, k), place).wait_recv()

    def weights(t):
        rows = pl.ds(pl.multiple_of(t * SPAN, SPAN), SPAN)
        slot = lax.rem(t, 2)
        return [pltpu.make_async_copy(w.at[rows, :], wbuf.at[slot, :, n * width : (n + 1) * width], wsem.at[slot, n])
                for n, w in enumerate((wq, wk, wv))]

    def loads(t, j):
        got = []
        for n, axes in enumerate(PARTS[j]):
            pair = pl.ds(beyond(me - core, axes), 2)
            got.append(pltpu.make_async_copy(g.at[t, pair], xbuf.at[j % 2, 2 * n : 2 * n + 2], xsem.at[j % 2, n]))
        return got

    def fetch(t, j):
        for axes in PARTS[j]:
            mates(t, axes, beyond(mate, axes))
        for c in loads(t, j):
            c.start()

    def own_loads(t):
        slot = lax.rem(t, 2)
        return [pltpu.make_async_copy(own(t, SPAN), xbuf.at[slot, core], xsem.at[slot, 0]),
                pltpu.make_async_copy(g.at[t, mate], xbuf.at[slot, 1 - core], xsem.at[slot, 1])]

    def own_fetch(t):
        mates(t, 7, mate)
        for c in own_loads(t):
            c.start()

    def add(slot, t, chips):
        for n, first in enumerate(chips):
            here = pl.ds(pl.multiple_of(first * per, 2 * per), 2 * per)
            acc[here, :] += _dot(xbuf[slot, 2 * n : 2 * n + 2].reshape(2 * per, SPAN), wbuf[lax.rem(t, 2)], 1, 0)

    def valid(p, f, *args):
        pl.when((p >= 0) & (p < pieces))(lambda: f(p, *args))

    for c in weights(0):
        c.start()
    lax.fori_loop(0, pieces, lambda p, _: across(p, 7, me, True).start(), None)
    acc[...] = jnp.zeros(acc.shape, jnp.float32)
    own_fetch(0)

    def turn_weights(t, more):
        for c in weights(t):
            c.wait()

        @pl.when(more)
        def _():
            for c in weights(lax.rem(t + 1, spans)):
                c.start()

    def step(i, _):
        t = i - before // SUBS
        for u in range(SUBS):
            for n, lag in AHEAD.items():
                if (u + lag - before) % turn == 0:
                    p = i * split + (u + lag - before) // turn
                    valid(p, begin) if n == "own" else valid(p, arrive, n)

            o = i * SUBS + u

            @pl.when(o < spans)
            def _():
                pl.when(o + 1 < spans)(lambda: own_fetch(o + 1))
                turn_weights(o, True)
                for c in own_loads(o):
                    c.wait()
                add(u % 2, o, [me - core])

            v = (u + 1) % SUBS
            ahead = t + (u + 1) // SUBS
            pl.when((ahead >= 0) & (ahead < spans))(lambda: fetch(ahead, v))

            @pl.when(t >= 0)
            def _():
                if u == 0:
                    turn_weights(t, t + 1 < spans)
                for c in loads(t, u):
                    c.wait()
                add(u % 2, t, [beyond(me - core, axes) for axes in PARTS[u]])

        return ()

    lax.fori_loop(0, spans + before // SUBS, step, ())

    def outs(j):
        slot = lax.rem(j, 2)
        at = pl.ds(pl.multiple_of(j * per, per), per)
        return [pltpu.make_async_copy(stage.at[slot, n * heads : (n + 1) * heads], out.at[:, at, :], osem.at[slot, n])
                for n, out in enumerate((q_out, k_out, v_out))]

    def finish(j, _):
        @pl.when(j >= 2)
        def _():
            for c in outs(j - 2):
                c.wait()

        here = pl.ds(pl.multiple_of(j * per, per), per)
        cos_n, sin_n, cos_f, sin_f = near_ref[0], near_ref[1], far_ref[0, pl.ds(j, 1), :], far_ref[1, pl.ds(j, 1), :]
        cos, sin = cos_n * cos_f - sin_n * sin_f, sin_n * cos_f + cos_n * sin_f
        sin = jnp.where(lax.broadcasted_iota(jnp.int32, sin.shape, 1) < HEAD // 2, -sin, sin)
        for i in range(3 * heads):
            t = acc[here, i * HEAD : (i + 1) * HEAD].astype(jnp.bfloat16)
            if i < 2 * heads:
                wide = t.astype(jnp.float32)
                t = (wide * cos + pltpu.roll(wide, HEAD // 2, 1) * sin).astype(jnp.bfloat16)
            stage[lax.rem(j, 2), i] = t
        for c in outs(j):
            c.start()
        return ()

    lax.fori_loop(0, group, finish, ())
    for j in (group - 2, group - 1):
        for c in outs(j):
            c.wait()

    def sent(p, _):
        for n in range(7):
            link(p, n, me).wait_send()
        for k in range(8):
            across(p, k, me).wait_send()
        return ()

    lax.fori_loop(0, pieces, sent, ())


def gather_project(h, wq, wk, wv, near, far, group):
    per, depth = h.shape
    width = wq.shape[1]
    heads = width // HEAD
    pieces = depth // PIECE
    before = -(-max(depth // SPAN, *AHEAD.values()) // SUBS) * SUBS
    anywhere, vmem = pl.BlockSpec(memory_space=pl.ANY), pl.BlockSpec(memory_space=pltpu.VMEM)
    out = jax.ShapeDtypeStruct((heads, group * per, HEAD), jnp.bfloat16)
    got = pl.pallas_call(
        functools.partial(_gather_project, pieces=pieces, before=before),
        in_specs=[anywhere] * 4 + [vmem] * 2,
        out_specs=[anywhere] * 4,
        out_shape=[out, out, out, jax.ShapeDtypeStruct((depth // SPAN, group, per, SPAN), jnp.bfloat16)],
        scratch_shapes=[
            pltpu.VMEM((group * per, 3 * width), jnp.float32),
            pltpu.VMEM((2, SPAN, 3 * width), jnp.bfloat16),
            pltpu.VMEM((2, 4, per, SPAN), jnp.bfloat16),
            pltpu.VMEM((2, 3 * heads, per, HEAD), jnp.bfloat16),
            pltpu.SemaphoreType.DMA((pieces, 7)),
            pltpu.SemaphoreType.DMA((pieces, 7)),
            pltpu.SemaphoreType.DMA((pieces, 8)),
            pltpu.SemaphoreType.DMA((pieces, 8)),
            pltpu.SemaphoreType.DMA((2, 3)),
            pltpu.SemaphoreType.DMA((2, 2)),
            pltpu.SemaphoreType.DMA((2, 3)),
        ],
        compiler_params=pltpu.CompilerParams(collective_id=0, has_side_effects=True, vmem_limit_bytes=VMEM),
        cost_estimate=pl.CostEstimate(
            flops=2 * group * per * depth * 3 * width, transcendentals=0, bytes_accessed=2 * (3 * wq.size + 3 * group * h.size)),
    )(h, wq, wk, wv, near, far)
    return got[:3]


def _attend(me_ref, q_ref, k_ref, v_ref, o_ref, top_s, mix_s, gap_s, *, scale, bq, bk):
    heads = q_ref.shape[0]
    iq = pl.program_id(0)
    e = scale * LOG2E
    top_s[...] = jnp.full(top_s.shape, NEG, jnp.float32)
    mix_s[...] = jnp.zeros(mix_s.shape, jnp.float32)
    gap_s[...] = lax.broadcasted_iota(jnp.int32, (bk, bq), 1) - lax.broadcasted_iota(jnp.int32, (bk, bq), 0)
    ones = jnp.ones((8, bk), jnp.bfloat16)

    def block(j, masked):
        here = pl.ds(j * bk, bk)
        scores = [_dot(k_ref[i, here, :], q_ref[i], 1, 1) for i in range(heads)]
        ok = gap_s[...] >= j * bk - iq * bq if masked else None
        weights, keeps = [], []
        for i, s in enumerate(scores):
            if masked:
                s = jnp.where(ok, s, HIDDEN)
            old = top_s[i : i + 1, :]
            top = jnp.maximum(old, s.max(axis=0, keepdims=True))
            top_s[i : i + 1, :] = top
            weights.append(jnp.exp2((s - top) * e).astype(jnp.bfloat16))
            keeps.append(jnp.exp2((old - top) * e))
        for i, (p, keep) in enumerate(zip(weights, keeps)):
            values = jnp.concatenate([v_ref[i, here, :].T, ones], axis=0)
            mix_s[i] = mix_s[i] * keep + _dot(values, p, 1, 0)

    whole = lax.div(iq * bq, bk)
    lax.fori_loop(0, whole, lambda j, _: block(j, False), None)
    lax.fori_loop(whole, lax.div(iq * bq + bq, bk), lambda j, _: block(j, True), None)

    low = lax.rem(me_ref[0], bq // 128)
    for i in range(heads):
        out = (mix_s[i, :HEAD, :] * (1 / mix_s[i, HEAD : HEAD + 1, :])).T.astype(jnp.bfloat16)
        for n in range(bq // 128):
            o_ref[jnp.bitwise_xor(low, n), :, i * HEAD : (i + 1) * HEAD] = out[n * 128 : (n + 1) * 128]


def attend(q, k, v, me, bq=512, bk=512):
    heads, tokens, _ = q.shape
    per = bq // 128
    whole = pl.BlockSpec((heads, tokens, HEAD), lambda i, me: (0, 0, 0))
    return pl.pallas_call(
        functools.partial(_attend, scale=HEAD**-0.5, bq=bq, bk=bk),
        grid_spec=pltpu.PrefetchScalarGridSpec(
            num_scalar_prefetch=1,
            grid=(tokens // bq,),
            in_specs=[pl.BlockSpec((heads, bq, HEAD), lambda i, me: (0, i, 0)), whole, whole],
            out_specs=pl.BlockSpec((per, 128, heads * HEAD), lambda i, me: (jnp.bitwise_xor(i, lax.div(me[0], per)), 0, 0)),
            scratch_shapes=[pltpu.VMEM((heads, bq), jnp.float32), pltpu.VMEM((heads, HEAD + 8, bq), jnp.float32),
                            pltpu.VMEM((bk, bq), jnp.int32)],
        ),
        out_shape=jax.ShapeDtypeStruct((tokens // 128, 128, heads * HEAD), jnp.bfloat16),
        compiler_params=pltpu.CompilerParams(dimension_semantics=("arbitrary",), vmem_limit_bytes=VMEM),
        cost_estimate=pl.CostEstimate(
            flops=2 * heads * tokens * tokens * HEAD, transcendentals=heads * tokens * tokens // 2, bytes_accessed=8 * q.size),
    )(me, q, k, v)


COUNT = (8, 4, 2, 1, 1)


def _project_scatter(seen, wo, x, y, r0, r1, r2, r3, wbuf, f0, f1, f2, f3, fx, s0, s1, s2, s3, s4, wsem, fsem, xsem, send, ysem, q0, q1, q2,
                     q3, *, pieces, lags, slots, early):
    me = lax.axis_index("tp")
    cols = wbuf.shape[2]
    arrived, fetches, stages, recv = (r0, r1, r2, r3), (f0, f1, f2, f3), (s0, s1, s2, s3, s4), (q0, q1, q2, q3)

    barrier = pltpu.get_barrier_semaphore()
    for w in (8, 4, 2, 1):
        pl.semaphore_signal(barrier, inc=1, device_id={"tp": _flip(me, w)}, device_id_type=pl.DeviceIdType.MESH)
    pl.semaphore_wait(barrier, 4)

    def here(p):
        return pl.ds(pl.multiple_of(p * cols, cols), cols)

    def weight(p):
        return pltpu.make_async_copy(wo.at[:, here(p)], wbuf.at[p], wsem.at[p])

    def out(p, k):
        slot = lax.rem(p, slots[k])
        if k == 4:
            return pltpu.make_async_copy(stages[4].at[slot], y.at[:, here(p)], ysem.at[slot])
        device = _flip(me, 1 if k == 0 else _axes(p)[k - 1])
        return pltpu.make_async_remote_copy(
            src_ref=stages[k].at[slot], dst_ref=arrived[k].at[p], send_sem=send.at[k, slot], recv_sem=recv[k].at[p],
            device_id={"tp": device}, device_id_type=pl.DeviceIdType.MESH)

    def share(k):
        first = COUNT[k] if k < 4 else 0
        return first, COUNT[k]

    def fetch(p, k):
        first, n = share(k)
        slot = lax.rem(p, 2)
        got = [pltpu.make_async_copy(arrived[m].at[p, first : first + n], fetches[m].at[slot, first : first + n], fsem.at[k, m, slot])
               for m in range(k)]
        if k == 4:
            got.append(pltpu.make_async_copy(x.at[:, here(p)], fx.at[slot], xsem.at[slot]))
        return got

    def ready(p, k):
        out(p, k - 1).wait_recv()
        for c in fetch(p, k):
            c.start()

    def work(p, k):
        first, n = share(k)
        w = _axes(p)
        js = []
        for i in range(n):
            i += first if k else 0
            if k == 0:
                js.append(1 + (i // 4) * w[0] + (i // 2 % 2) * w[1] + (i % 2) * w[2])
            else:
                js.append((i // 4) * w[0] + (i // 2 % 2) * w[1] + (i % 2) * w[2])
        rows = jnp.concatenate([seen[j] for j in js], axis=0) if n > 1 else seen[js[0]]
        total = _dot(rows, wbuf[p], 1, 0)
        slot = lax.rem(p, 2)
        if k:
            for c in fetch(p, k):
                c.wait()
            for m in range(k):
                total += fetches[m][slot, first : first + n].reshape(total.shape).astype(jnp.float32)
        if k == 4:
            total = fx[slot].astype(jnp.float32) + total

        @pl.when(p >= slots[k])
        def _():
            c = out(p - slots[k], k)
            c.wait() if k == 4 else c.wait_send()

        at = stages[k].at[lax.rem(p, slots[k])]
        at[...] = total.astype(jnp.bfloat16).reshape(at.shape)
        out(p, k).start()

    def valid(p, f, *args):
        pl.when((p >= 0) & (p < pieces))(lambda: f(p, *args))

    for p in range(early):
        weight(p).start()

    def step(i, _):
        for k in (3, 2, 1, 4):
            valid(i - lags[k], work, k)
        for k in (4, 3, 2, 1):
            valid(i + 1 - lags[k], ready, k)

        def begin(p):
            pl.when(p + early < pieces)(lambda: weight(p + early).start())
            weight(p).wait()
            work(p, 0)

        valid(i, begin)
        return ()

    lax.fori_loop(0, pieces + lags[4], step, ())
    for k in range(5):
        for p in range(pieces - slots[k], pieces):
            c = out(p, k)
            c.wait() if k == 4 else c.wait_send()


def project_scatter(seen, wo, x):
    per, width = seen.shape[1:]
    depth = wo.shape[1]
    pieces = depth // TURN
    anywhere, vmem = pl.BlockSpec(memory_space=pl.ANY), pl.BlockSpec(memory_space=pltpu.VMEM)
    arrivals = [jax.ShapeDtypeStruct((pieces, n, per, TURN), jnp.bfloat16) for n in COUNT[:4]]
    got = pl.pallas_call(
        functools.partial(_project_scatter, pieces=pieces, lags=LAGS, slots=SLOTS, early=4),
        in_specs=[vmem, anywhere, anywhere],
        out_specs=[anywhere] * 5,
        out_shape=[jax.ShapeDtypeStruct(x.shape, x.dtype), *arrivals],
        scratch_shapes=[pltpu.VMEM((pieces, width, TURN), jnp.bfloat16)]
        + [pltpu.VMEM((2, n, per, TURN), jnp.bfloat16) for n in COUNT[:4]]
        + [pltpu.VMEM((2, per, TURN), jnp.bfloat16)]
        + [pltpu.VMEM((slots, n, per, TURN), jnp.bfloat16) for slots, n in zip(SLOTS[:4], COUNT[:4])]
        + [pltpu.VMEM((SLOTS[4], per, TURN), jnp.bfloat16)]
        + [pltpu.SemaphoreType.DMA((pieces,)), pltpu.SemaphoreType.DMA((5, 4, 2)), pltpu.SemaphoreType.DMA((2,)),
           pltpu.SemaphoreType.DMA((4, max(SLOTS))), pltpu.SemaphoreType.DMA((SLOTS[4],))]
        + [pltpu.SemaphoreType.DMA((pieces,)) for _ in range(4)],
        compiler_params=pltpu.CompilerParams(collective_id=1, has_side_effects=True, vmem_limit_bytes=VMEM),
        cost_estimate=pl.CostEstimate(flops=2 * 16 * per * width * depth, transcendentals=0, bytes_accessed=2 * (wo.size + 32 * x.size)),
    )(seen, wo, x)
    return got[0]


def solution(mesh):
    group = mesh.shape["tp"]

    def step(x, gain, wq, wk, wv, wo):
        per, depth = x.shape
        me = lax.axis_index("tp")
        half = HEAD // 2
        place = jnp.concatenate([jnp.arange(per), jnp.arange(group) * per]).astype(jnp.float32)
        angle = place[:, None] * THETA ** (-jnp.arange(half, dtype=jnp.float32) / half)
        turn = jnp.stack([jnp.cos(angle), jnp.sin(angle)])
        turn = jnp.concatenate([turn, turn], -1)
        q, k, v = gather_project(normed(x, gain), wq, wk, wv, turn[:, :per], turn[:, per:], group)
        seen = attend(q, k, v, me.astype(jnp.int32).reshape(1))
        return project_scatter(seen, wo, x)

    tokens, columns = P(("dp", "tp"), None), P(None, "tp")
    return jax.shard_map(
        step,
        mesh=mesh,
        in_specs=(tokens, P(None), columns, columns, columns, P("tp", None)),
        out_specs=tokens,
        check_vma=False,
    )
```

```python
import functools

import jax
import jax.numpy as jnp
from jax import lax
from jax.experimental import pallas as pl
from jax.experimental.pallas import tpu as pltpu
from jax.sharding import PartitionSpec as P

NEG = -1e30
HIDDEN = 2 * NEG
LOG2E = 1.4426950408889634
VMEM = 56 * 2**20
HEAD = 128
THETA = 10000
SPAN = 1024
PIECE = 512
PARTS = (((0,), (1,)), ((2,), (0, 1)), ((1, 2), (0, 2)), ((0, 1, 2),))
SUBS = 4
AHEAD = {"own": 16, 0: 10, 1: 10, 2: 5, 6: 1, 3: 7, 4: 5, 5: 4}
TURN = 512
LAGS = (0, 2, 6, 9, 12)
SLOTS = (3, 6, 4, 4, 2)


def _dot(a, b, ca, cb):
    return lax.dot_general(a, b, (((ca,), (cb,)), ((), ())), preferred_element_type=jnp.float32)


def _norm(x_ref, gain_ref, o_ref):
    wide = x_ref[...].astype(jnp.float32)
    scale = lax.rsqrt(jnp.mean(wide * wide, -1, keepdims=True) + 1e-6)
    o_ref[...] = (wide * scale * gain_ref[...].astype(jnp.float32)).astype(o_ref.dtype)


def normed(x, gain, rows=32):
    depth = x.shape[1]
    block = pl.BlockSpec((rows, depth), lambda i: (i, 0))
    return pl.pallas_call(
        _norm,
        grid=(x.shape[0] // rows,),
        in_specs=[block, pl.BlockSpec((1, depth), lambda i: (0, 0))],
        out_specs=block,
        out_shape=jax.ShapeDtypeStruct(x.shape, jnp.bfloat16),
        compiler_params=pltpu.CompilerParams(dimension_semantics=("arbitrary",), vmem_limit_bytes=VMEM // 2),
        cost_estimate=pl.CostEstimate(flops=4 * x.size, transcendentals=x.shape[0], bytes_accessed=4 * x.size),
    )(x, gain.reshape(1, -1))


def _flip(place, weight):
    return place + weight * (1 - 2 * lax.rem(lax.div(place, weight), 2))


def _axes(piece):
    turns = [lax.rem(piece + n, 3) for n in range(3)]
    return [lax.div(8, 1 + r + lax.div(r, 2)) for r in turns]


PATHS = ((0,), (1,), (0, 1), (2,), (0, 2), (1, 2), (0, 1, 2))
ONWARD = {0: (2, 4), 1: (5,), 2: (6,)}


def _gather_project(h, wq, wk, wv, near_ref, far_ref, q_out, k_out, v_out, g, acc, wbuf, xbuf, stage, send, recv, core_send, core_recv,
                    wsem, xsem, osem, *, pieces, before):
    me = lax.axis_index("tp")
    mate = _flip(me, 1)
    spans, group, per, _ = g.shape
    split = pieces // spans
    turn = SUBS // split
    width = wq.shape[1]
    heads = width // HEAD
    core = lax.rem(me, 2)

    barrier = pltpu.get_barrier_semaphore()
    for w in (8, 4, 2, 1):
        pl.semaphore_signal(barrier, inc=1, device_id={"tp": _flip(me, w)}, device_id_type=pl.DeviceIdType.MESH)
    pl.semaphore_wait(barrier, 4)

    def own(p, size=PIECE):
        return h.at[:, pl.ds(pl.multiple_of(p * size, size), size)]

    def held(p, block):
        return g.at[lax.div(p, split), block, :, pl.ds(pl.multiple_of(lax.rem(p, split) * PIECE, PIECE), PIECE)]

    def remote(src, dst, ssem, rsem, device):
        return pltpu.make_async_remote_copy(src_ref=src, dst_ref=dst, send_sem=ssem, recv_sem=rsem, device_id={"tp": device},
                                            device_id_type=pl.DeviceIdType.MESH)

    def block_of(place, p, n):
        w = _axes(p)
        for step in PATHS[n]:
            place = _flip(place, w[step])
        return place

    def link(p, n, block, mine=False):
        device = _flip(me, _axes(p)[PATHS[n][-1]])
        return remote(own(p) if mine else held(p, block), held(p, block), send.at[p, n], recv.at[p, n], device)

    def across(p, k, block, mine=False):
        return remote(own(p) if mine else held(p, block), held(p, block), core_send.at[p, k], core_recv.at[p, k], mate)

    def begin(p):
        for n in (0, 1, 3):
            link(p, n, me, True).start()

    def arrive(p, n):
        block = block_of(me, p, n)
        link(p, n, block).wait_recv()
        for m in ONWARD.get(n, ()):
            link(p, m, block).start()
        across(p, n, block).start()

    def beyond(place, axes):
        for axis in axes:
            place = _flip(place, (8, 4, 2)[axis])
        return place

    def number(p, axes):
        if len(axes) == 3:
            return 6
        axis = axes[0] if len(axes) == 1 else 3 - sum(axes)
        turn = lax.rem(axis + 3 - lax.rem(p, 3), 3)
        bend = turn + lax.div(turn, 2)
        return bend if len(axes) == 1 else 5 - bend

    def mates(t, k, place):
        for n in range(split):
            across(t * split + n, k if isinstance(k, int) else number(t * split + n, k), place).wait_recv()

    def weights(turn):
        rows = pl.ds(pl.multiple_of(lax.rem(turn, spans) * SPAN, SPAN), SPAN)
        slot = lax.rem(turn, 3)
        return [pltpu.make_async_copy(w.at[rows, :], wbuf.at[slot, :, n * width : (n + 1) * width], wsem.at[slot, n])
                for n, w in enumerate((wq, wk, wv))]

    def loads(t, j):
        got = []
        for n, axes in enumerate(PARTS[j]):
            pair = pl.ds(beyond(me - core, axes), 2)
            got.append(pltpu.make_async_copy(g.at[t, pair], xbuf.at[j % 2, 2 * n : 2 * n + 2], xsem.at[j % 2, n]))
        return got

    def fetch(t, j):
        for axes in PARTS[j]:
            mates(t, axes, beyond(mate, axes))
        for c in loads(t, j):
            c.start()

    def own_loads(t):
        slot = lax.rem(t, 2)
        return [pltpu.make_async_copy(own(t, SPAN), xbuf.at[slot, core], xsem.at[slot, 0]),
                pltpu.make_async_copy(g.at[t, mate], xbuf.at[slot, 1 - core], xsem.at[slot, 1])]

    def own_fetch(t):
        mates(t, 7, mate)
        for c in own_loads(t):
            c.start()

    def add(slot, turn, chips):
        for n, first in enumerate(chips):
            here = pl.ds(pl.multiple_of(first * per, 2 * per), 2 * per)
            acc[here, :] += _dot(xbuf[slot, 2 * n : 2 * n + 2].reshape(2 * per, SPAN), wbuf[lax.rem(turn, 3)], 1, 0)

    def valid(p, f, *args):
        pl.when((p >= 0) & (p < pieces))(lambda: f(p, *args))

    for c in weights(0) + weights(1):
        c.start()
    lax.fori_loop(0, pieces, lambda p, _: across(p, 7, me, True).start(), None)
    acc[...] = jnp.zeros(acc.shape, jnp.float32)
    own_fetch(0)

    def take_weights(turn):
        for c in weights(turn):
            c.wait()

        @pl.when(turn + 2 < 2 * spans)
        def _():
            for c in weights(turn + 2):
                c.start()

    def step(i, _):
        t = i - before // SUBS
        for u in range(SUBS):
            for n, lag in AHEAD.items():
                if (u + lag - before) % turn == 0:
                    p = i * split + (u + lag - before) // turn
                    valid(p, begin) if n == "own" else valid(p, arrive, n)

            o = i * SUBS + u

            @pl.when(o < spans)
            def _():
                pl.when(o + 1 < spans)(lambda: own_fetch(o + 1))
                take_weights(o)
                for c in own_loads(o):
                    c.wait()
                add(u % 2, o, [me - core])

            v = (u + 1) % SUBS
            ahead = t + (u + 1) // SUBS
            pl.when((ahead >= 0) & (ahead < spans))(lambda: fetch(ahead, v))

            @pl.when(t >= 0)
            def _():
                if u == 0:
                    take_weights(spans + t)
                for c in loads(t, u):
                    c.wait()
                add(u % 2, spans + t, [beyond(me - core, axes) for axes in PARTS[u]])

        return ()

    lax.fori_loop(0, spans + before // SUBS, step, ())

    def outs(j):
        slot = lax.rem(j, 2)
        at = pl.ds(pl.multiple_of(j * per, per), per)
        return [pltpu.make_async_copy(stage.at[slot, n * heads : (n + 1) * heads], out.at[:, at, :], osem.at[slot, n])
                for n, out in enumerate((q_out, k_out, v_out))]

    def finish(j, _):
        @pl.when(j >= 2)
        def _():
            for c in outs(j - 2):
                c.wait()

        here = pl.ds(pl.multiple_of(j * per, per), per)
        cos_n, sin_n, cos_f, sin_f = near_ref[0], near_ref[1], far_ref[0, pl.ds(j, 1), :], far_ref[1, pl.ds(j, 1), :]
        cos, sin = cos_n * cos_f - sin_n * sin_f, sin_n * cos_f + cos_n * sin_f
        sin = jnp.where(lax.broadcasted_iota(jnp.int32, sin.shape, 1) < HEAD // 2, -sin, sin)
        for i in range(3 * heads):
            t = acc[here, i * HEAD : (i + 1) * HEAD].astype(jnp.bfloat16)
            if i < 2 * heads:
                wide = t.astype(jnp.float32)
                t = (wide * cos + pltpu.roll(wide, HEAD // 2, 1) * sin).astype(jnp.bfloat16)
            stage[lax.rem(j, 2), i] = t
        for c in outs(j):
            c.start()
        return ()

    lax.fori_loop(0, group, finish, ())
    for j in (group - 2, group - 1):
        for c in outs(j):
            c.wait()

    def sent(p, _):
        for n in range(7):
            link(p, n, me).wait_send()
        for k in range(8):
            across(p, k, me).wait_send()
        return ()

    lax.fori_loop(0, pieces, sent, ())


def gather_project(h, wq, wk, wv, near, far, group):
    per, depth = h.shape
    width = wq.shape[1]
    heads = width // HEAD
    pieces = depth // PIECE
    before = -(-max(depth // SPAN, *AHEAD.values()) // SUBS) * SUBS
    anywhere, vmem = pl.BlockSpec(memory_space=pl.ANY), pl.BlockSpec(memory_space=pltpu.VMEM)
    out = jax.ShapeDtypeStruct((heads, group * per, HEAD), jnp.bfloat16)
    got = pl.pallas_call(
        functools.partial(_gather_project, pieces=pieces, before=before),
        in_specs=[anywhere] * 4 + [vmem] * 2,
        out_specs=[anywhere] * 4,
        out_shape=[out, out, out, jax.ShapeDtypeStruct((depth // SPAN, group, per, SPAN), jnp.bfloat16)],
        scratch_shapes=[
            pltpu.VMEM((group * per, 3 * width), jnp.float32),
            pltpu.VMEM((3, SPAN, 3 * width), jnp.bfloat16),
            pltpu.VMEM((2, 4, per, SPAN), jnp.bfloat16),
            pltpu.VMEM((2, 3 * heads, per, HEAD), jnp.bfloat16),
            pltpu.SemaphoreType.DMA((pieces, 7)),
            pltpu.SemaphoreType.DMA((pieces, 7)),
            pltpu.SemaphoreType.DMA((pieces, 8)),
            pltpu.SemaphoreType.DMA((pieces, 8)),
            pltpu.SemaphoreType.DMA((3, 3)),
            pltpu.SemaphoreType.DMA((2, 2)),
            pltpu.SemaphoreType.DMA((2, 3)),
        ],
        compiler_params=pltpu.CompilerParams(collective_id=0, has_side_effects=True, vmem_limit_bytes=VMEM),
        cost_estimate=pl.CostEstimate(
            flops=2 * group * per * depth * 3 * width, transcendentals=0, bytes_accessed=2 * (3 * wq.size + 3 * group * h.size)),
    )(h, wq, wk, wv, near, far)
    return got[:3]


def _attend(me_ref, q_ref, k_ref, v_ref, o_ref, top_s, mix_s, gap_s, *, scale, bq, bk):
    heads = q_ref.shape[0]
    iq = pl.program_id(0)
    e = scale * LOG2E
    top_s[...] = jnp.full(top_s.shape, NEG, jnp.float32)
    mix_s[...] = jnp.zeros(mix_s.shape, jnp.float32)
    gap_s[...] = lax.broadcasted_iota(jnp.int32, (bk, bq), 1) - lax.broadcasted_iota(jnp.int32, (bk, bq), 0)
    ones = jnp.ones((8, bk), jnp.bfloat16)

    def block(j, masked):
        here = pl.ds(j * bk, bk)
        scores = [_dot(k_ref[i, here, :], q_ref[i], 1, 1) for i in range(heads)]
        ok = gap_s[...] >= j * bk - iq * bq if masked else None
        weights, keeps = [], []
        for i, s in enumerate(scores):
            if masked:
                s = jnp.where(ok, s, HIDDEN)
            old = top_s[i : i + 1, :]
            top = jnp.maximum(old, s.max(axis=0, keepdims=True))
            top_s[i : i + 1, :] = top
            weights.append(jnp.exp2((s - top) * e).astype(jnp.bfloat16))
            keeps.append(jnp.exp2((old - top) * e))
        for i, (p, keep) in enumerate(zip(weights, keeps)):
            values = jnp.concatenate([v_ref[i, here, :].T, ones], axis=0)
            mix_s[i] = mix_s[i] * keep + _dot(values, p, 1, 0)

    whole = lax.div(iq * bq, bk)
    lax.fori_loop(0, whole, lambda j, _: block(j, False), None)
    lax.fori_loop(whole, lax.div(iq * bq + bq, bk), lambda j, _: block(j, True), None)

    low = lax.rem(me_ref[0], bq // 128)
    for i in range(heads):
        out = (mix_s[i, :HEAD, :] * (1 / mix_s[i, HEAD : HEAD + 1, :])).T.astype(jnp.bfloat16)
        for n in range(bq // 128):
            o_ref[jnp.bitwise_xor(low, n), :, i * HEAD : (i + 1) * HEAD] = out[n * 128 : (n + 1) * 128]


def attend(q, k, v, me, bq=512, bk=512):
    heads, tokens, _ = q.shape
    per = bq // 128
    whole = pl.BlockSpec((heads, tokens, HEAD), lambda i, me: (0, 0, 0))
    return pl.pallas_call(
        functools.partial(_attend, scale=HEAD**-0.5, bq=bq, bk=bk),
        grid_spec=pltpu.PrefetchScalarGridSpec(
            num_scalar_prefetch=1,
            grid=(tokens // bq,),
            in_specs=[pl.BlockSpec((heads, bq, HEAD), lambda i, me: (0, i, 0)), whole, whole],
            out_specs=pl.BlockSpec((per, 128, heads * HEAD), lambda i, me: (jnp.bitwise_xor(i, lax.div(me[0], per)), 0, 0)),
            scratch_shapes=[pltpu.VMEM((heads, bq), jnp.float32), pltpu.VMEM((heads, HEAD + 8, bq), jnp.float32),
                            pltpu.VMEM((bk, bq), jnp.int32)],
        ),
        out_shape=jax.ShapeDtypeStruct((tokens // 128, 128, heads * HEAD), jnp.bfloat16),
        compiler_params=pltpu.CompilerParams(dimension_semantics=("arbitrary",), vmem_limit_bytes=VMEM),
        cost_estimate=pl.CostEstimate(
            flops=2 * heads * tokens * tokens * HEAD, transcendentals=heads * tokens * tokens // 2, bytes_accessed=8 * q.size),
    )(me, q, k, v)


COUNT = (8, 4, 2, 1, 1)


def _project_scatter(seen, wo, x, y, r0, r1, r2, r3, wbuf, f0, f1, f2, f3, fx, s0, s1, s2, s3, s4, wsem, fsem, xsem, send, ysem, q0, q1, q2,
                     q3, *, pieces, lags, slots, early):
    me = lax.axis_index("tp")
    cols = wbuf.shape[2]
    arrived, fetches, stages, recv = (r0, r1, r2, r3), (f0, f1, f2, f3), (s0, s1, s2, s3, s4), (q0, q1, q2, q3)

    barrier = pltpu.get_barrier_semaphore()
    for w in (8, 4, 2, 1):
        pl.semaphore_signal(barrier, inc=1, device_id={"tp": _flip(me, w)}, device_id_type=pl.DeviceIdType.MESH)
    pl.semaphore_wait(barrier, 4)

    def here(p):
        return pl.ds(pl.multiple_of(p * cols, cols), cols)

    def weight(p):
        return pltpu.make_async_copy(wo.at[:, here(p)], wbuf.at[p], wsem.at[p])

    def out(p, k):
        slot = lax.rem(p, slots[k])
        if k == 4:
            return pltpu.make_async_copy(stages[4].at[slot], y.at[:, here(p)], ysem.at[slot])
        device = _flip(me, 1 if k == 0 else _axes(p)[k - 1])
        return pltpu.make_async_remote_copy(
            src_ref=stages[k].at[slot], dst_ref=arrived[k].at[p], send_sem=send.at[k, slot], recv_sem=recv[k].at[p],
            device_id={"tp": device}, device_id_type=pl.DeviceIdType.MESH)

    def share(k):
        first = COUNT[k] if k < 4 else 0
        return first, COUNT[k]

    def fetch(p, k):
        first, n = share(k)
        slot = lax.rem(p, 2)
        got = [pltpu.make_async_copy(arrived[m].at[p, first : first + n], fetches[m].at[slot, first : first + n], fsem.at[k, m, slot])
               for m in range(k)]
        if k == 4:
            got.append(pltpu.make_async_copy(x.at[:, here(p)], fx.at[slot], xsem.at[slot]))
        return got

    def ready(p, k):
        out(p, k - 1).wait_recv()
        for c in fetch(p, k):
            c.start()

    def work(p, k):
        first, n = share(k)
        w = _axes(p)
        js = []
        for i in range(n):
            i += first if k else 0
            if k == 0:
                js.append(1 + (i // 4) * w[0] + (i // 2 % 2) * w[1] + (i % 2) * w[2])
            else:
                js.append((i // 4) * w[0] + (i // 2 % 2) * w[1] + (i % 2) * w[2])
        rows = jnp.concatenate([seen[j] for j in js], axis=0) if n > 1 else seen[js[0]]
        total = _dot(rows, wbuf[p], 1, 0)
        slot = lax.rem(p, 2)
        if k:
            for c in fetch(p, k):
                c.wait()
            for m in range(k):
                total += fetches[m][slot, first : first + n].reshape(total.shape).astype(jnp.float32)
        if k == 4:
            total = fx[slot].astype(jnp.float32) + total

        @pl.when(p >= slots[k])
        def _():
            c = out(p - slots[k], k)
            c.wait() if k == 4 else c.wait_send()

        at = stages[k].at[lax.rem(p, slots[k])]
        at[...] = total.astype(jnp.bfloat16).reshape(at.shape)
        out(p, k).start()

    def valid(p, f, *args):
        pl.when((p >= 0) & (p < pieces))(lambda: f(p, *args))

    for p in range(early):
        weight(p).start()

    def step(i, _):
        for k in (3, 2, 1, 4):
            valid(i - lags[k], work, k)
        for k in (4, 3, 2, 1):
            valid(i + 1 - lags[k], ready, k)

        def begin(p):
            pl.when(p + early < pieces)(lambda: weight(p + early).start())
            weight(p).wait()
            work(p, 0)

        valid(i, begin)
        return ()

    lax.fori_loop(0, pieces + lags[4], step, ())
    for k in range(5):
        for p in range(pieces - slots[k], pieces):
            c = out(p, k)
            c.wait() if k == 4 else c.wait_send()


def project_scatter(seen, wo, x):
    per, width = seen.shape[1:]
    depth = wo.shape[1]
    pieces = depth // TURN
    anywhere, vmem = pl.BlockSpec(memory_space=pl.ANY), pl.BlockSpec(memory_space=pltpu.VMEM)
    arrivals = [jax.ShapeDtypeStruct((pieces, n, per, TURN), jnp.bfloat16) for n in COUNT[:4]]
    got = pl.pallas_call(
        functools.partial(_project_scatter, pieces=pieces, lags=LAGS, slots=SLOTS, early=4),
        in_specs=[vmem, anywhere, anywhere],
        out_specs=[anywhere] * 5,
        out_shape=[jax.ShapeDtypeStruct(x.shape, x.dtype), *arrivals],
        scratch_shapes=[pltpu.VMEM((pieces, width, TURN), jnp.bfloat16)]
        + [pltpu.VMEM((2, n, per, TURN), jnp.bfloat16) for n in COUNT[:4]]
        + [pltpu.VMEM((2, per, TURN), jnp.bfloat16)]
        + [pltpu.VMEM((slots, n, per, TURN), jnp.bfloat16) for slots, n in zip(SLOTS[:4], COUNT[:4])]
        + [pltpu.VMEM((SLOTS[4], per, TURN), jnp.bfloat16)]
        + [pltpu.SemaphoreType.DMA((pieces,)), pltpu.SemaphoreType.DMA((5, 4, 2)), pltpu.SemaphoreType.DMA((2,)),
           pltpu.SemaphoreType.DMA((4, max(SLOTS))), pltpu.SemaphoreType.DMA((SLOTS[4],))]
        + [pltpu.SemaphoreType.DMA((pieces,)) for _ in range(4)],
        compiler_params=pltpu.CompilerParams(collective_id=1, has_side_effects=True, vmem_limit_bytes=VMEM),
        cost_estimate=pl.CostEstimate(flops=2 * 16 * per * width * depth, transcendentals=0, bytes_accessed=2 * (wo.size + 32 * x.size)),
    )(seen, wo, x)
    return got[0]


def solution(mesh):
    group = mesh.shape["tp"]

    def step(x, gain, wq, wk, wv, wo):
        per, depth = x.shape
        me = lax.axis_index("tp")
        half = HEAD // 2
        place = jnp.concatenate([jnp.arange(per), jnp.arange(group) * per]).astype(jnp.float32)
        angle = place[:, None] * THETA ** (-jnp.arange(half, dtype=jnp.float32) / half)
        turn = jnp.stack([jnp.cos(angle), jnp.sin(angle)])
        turn = jnp.concatenate([turn, turn], -1)
        q, k, v = gather_project(normed(x, gain), wq, wk, wv, turn[:, :per], turn[:, per:], group)
        seen = attend(q, k, v, me.astype(jnp.int32).reshape(1))
        return project_scatter(seen, wo, x)

    tokens, columns = P(("dp", "tp"), None), P(None, "tp")
    return jax.shard_map(
        step,
        mesh=mesh,
        in_specs=(tokens, P(None), columns, columns, columns, P("tp", None)),
        out_specs=tokens,
        check_vma=False,
    )
```
